32 devices in a mesh: dp: 4 (over y, core), expert: 4 (over z), pipe: 2 (over x).
Axes of the slice: x: 2, y: 2, z: 4, core: 2. Of those that a mesh axis runs over, the one named last changes fastest.
Arguments:
- inputs: bfloat16 [512, 4096], P('expert'), may hold values from -6 to 6
- cotangents: bfloat16 [512, 4096], P('expert'), may hold values from -6 to 6
- routes: int32 [512, 2], P('expert'), may hold values from 0 to 3, all different within a row; in each aligned block of 128 rows (0 to 127, 128 to 255, ...) at most 128 rows name the same one
- gates: float32 [512, 2], P('expert'), may hold values from 0.1 to 1
- w_gate: bfloat16 [4, 4096, 7168], P('expert', None, ('dp', 'pipe')), may hold values from -0.09375 to 0.09375
- w_up: bfloat16 [4, 4096, 7168], P('expert', None, ('dp', 'pipe')), may hold values from -0.09375 to 0.09375
- w_down: bfloat16 [4, 7168, 4096], P('expert', ('dp', 'pipe')), may hold values from -0.09375 to 0.09375
- proj_in: bfloat16 [4096, 32], replicated, may hold values from -0.09375 to 0.09375
- proj_out: bfloat16 [4096, 64], replicated, may hold values from -0.09375 to 0.09375
- proj_hid_a: bfloat16 [7168, 32], P(('dp', 'pipe')), may hold values from -0.0625 to 0.0625
- proj_hid_b: bfloat16 [7168, 64], P(('dp', 'pipe')), may hold values from -0.0625 to 0.0625
- queries: bfloat16 [256, 6144], P(('dp', 'pipe')), may hold values from -0.078125 to 0.078125
Outputs:
- token_scores: float32 [512, 256], P('expert', ('dp', 'pipe'))
- query_totals: float32 [256], P(('dp', 'pipe'))
The draws below stay inside these ranges and needn't reach their ends.
Inputs may be any that keep to these rules, and one draw needn't show every extreme that they name: `routes`: each row names two different experts. Among the 128 tokens of one index of expert (aligned blocks), no expert is named more than 128 times, and in some blocks one expert is named exactly 128 times.
All inputs are finite; a program needn't handle non-finite values.
Results may differ from the reference program's by a relative error of at most 0.0041.
Values may be sent and summed in bfloat16 or wider, within the bound.
No kernel may reach another device: no remote copies, remote signals or barrier semaphores. Data moves between devices by JAX's collectives and lax.ppermute only.
A program may use at most 128 MiB of HBM per device.

```python
import math
import jax
import jax.numpy as jnp
import numpy as np
from jax import lax

D = 4096
FF = 7168
KA = 32
KB = 64
NQ = 256
TOK_DEV = 128
EXPERTS = 4
TOKENS = 512
CAP = 128
SKETCH = 6144
N_EXPERT = 4


def block_levels(stream_key, extent, pieces, low, top_value):
    def one(dim, shards_of):
        steps = jax.random.uniform(jax.random.fold_in(jax.random.fold_in(stream_key, 6), dim), (shards_of,), jnp.float32, low / len(pieces), top_value / len(pieces))
        return jnp.repeat(jnp.exp(steps), extent[dim] // shards_of).reshape((-1,) + (1,) * (len(extent) - dim - 1))

    gain = one(*pieces[0])
    for cut in pieces[1:]:
        gain = gain * one(*cut)
    return gain


def shared_out(stream_key, own, number, rows, count, top, bound, skew):
    order = jax.random.permutation(stream_key, count)
    crowded, common = portions_of(count, rows * top, bound, skew, True), portions_of(count, rows * top, bound, skew, False)
    places = jnp.arange(count)

    def named(sizes, rotation):
        used = int((sizes > 0).sum())
        fixed = max(1, used // 4)
        passed = fixed + (places - fixed + rotation * (used - fixed)) % max(1, count - fixed)
        return jnp.zeros((count,), jnp.int32).at[order[jnp.where(places < fixed, places, passed)]].set(jnp.asarray(sizes, jnp.int32))

    sizes = jnp.where(number % 4 == 0, named(crowded, number // 4), named(common, number - number // 4 - 1))
    mixed = jax.random.permutation(jax.random.fold_in(own, 3), count)
    source_of, taker = mixed[0:count // 2 * 2:2], mixed[1:count // 2 * 2:2]
    room = jnp.minimum(sizes[source_of] - 1, bound - sizes[taker]) // 2
    room = jnp.where((source_of == order[0]) | (taker == order[0]) | (sizes[taker] == 0), 0, jnp.maximum(room, 0))
    passed = jax.random.randint(jax.random.fold_in(own, 4), (count // 2,), 0, 1 << 20) % (room + 1)
    sizes = sizes.at[source_of].add(-passed).at[taker].add(passed)
    items = jnp.searchsorted(jnp.cumsum(sizes), jnp.arange(rows * top), side="right").astype(jnp.int32)
    table = items.reshape(top, rows).T
    table = table[jax.random.permutation(jax.random.fold_in(own, 1), rows)]
    rotation = jax.random.randint(jax.random.fold_in(own, 2), (rows, 1), 0, top)
    return jnp.take_along_axis(table, (jnp.arange(top)[None, :] + rotation) % top, axis=1)


def portions_of(count, total, bound, slope, full):
    loads = [(1 << 20) // math.isqrt(rank ** slope) + 1 for rank in range(1, count + 1)]
    largest = bound if full else min(bound, max(-(-total // count), total * loads[0] // sum(loads)))
    least = 1 if total - largest >= count - 1 else 0
    given, surplus = [largest] + [least] * (count - 1), total - largest - least * (count - 1)
    while surplus > 0:
        candidates = [i for i in range(1, count) if given[i] < largest] or [i for i in range(1, count) if given[i] < bound]
        pool, left = sum([loads[i] for i in candidates]), surplus
        for i in candidates:
            more = min(bound - given[i], max(1, left * loads[i] // pool), surplus)
            given[i] = given[i] + more
            surplus = surplus - more
    return np.array(given)


def scatter_about(rng, dims, deviation, most, shards=(), kind=jnp.bfloat16):
    drawn = deviation * jax.random.normal(rng, dims, jnp.float32)
    if shards:
        drawn = drawn * block_levels(rng, dims, shards, -0.22, 0.18)
    return jnp.clip(drawn, -most, most).astype(kind)


def setup_inputs(seed: int = 0) -> dict:
    splits = jax.random.split(jax.random.key(seed), 13)
    inputs = scatter_about(splits[0], (TOKENS, D), 1.0, 6.0, ((0, 4),))
    cotangents = scatter_about(splits[1], (TOKENS, D), 1.0, 6.0, ((0, 4),))
    routes_keys = jax.random.split(jax.random.fold_in(splits[2], 1), TOKENS // TOK_DEV)
    routes_turns = jax.random.permutation(jax.random.fold_in(splits[2], 3), TOKENS // TOK_DEV)
    routes = jax.vmap(lambda own, number: shared_out(jax.random.fold_in(splits[2], 2), own, number, TOK_DEV, EXPERTS, 2, CAP, 2))(routes_keys, routes_turns).reshape((TOKENS, 2))
    gates = jnp.clip(jnp.exp(math.log(1.0) - 2.3025851 * jax.random.uniform(splits[3], (TOKENS, 2), jnp.float32) ** block_levels(splits[3], (TOKENS, 2), ((0, 4),), -0.2, 0.2)), 0.1, 1.0)
    w_gate = scatter_about(splits[4], (EXPERTS, D, FF), D ** -0.5, 0.09375, ((0, 4), (2, 8)))
    w_up = scatter_about(splits[5], (EXPERTS, D, FF), D ** -0.5, 0.09375, ((0, 4), (2, 8)))
    w_down = scatter_about(splits[6], (EXPERTS, FF, D), D ** -0.5, 0.09375, ((0, 4), (1, 8)))
    proj_in = scatter_about(splits[7], (D, KA), D ** -0.5, 0.09375)
    proj_out = scatter_about(splits[8], (D, KB), D ** -0.5, 0.09375)
    proj_hid_a = scatter_about(splits[9], (FF, KA), FF ** -0.5, 0.0625, ((0, 8),))
    proj_hid_b = scatter_about(splits[10], (FF, KB), FF ** -0.5, 0.0625, ((0, 8),))
    queries = scatter_about(splits[11], (NQ, SKETCH), SKETCH ** -0.5, 0.078125, ((0, 8),))
    return dict(inputs=inputs, cotangents=cotangents, routes=routes, gates=gates, w_gate=w_gate, w_up=w_up, w_down=w_down, proj_in=proj_in, proj_out=proj_out, proj_hid_a=proj_hid_a, proj_hid_b=proj_hid_b, queries=queries)


def slot_matrix(route_rows, gate_rows, experts, capacity):
    count = route_rows.shape[0]
    flat = route_rows.reshape(-1)
    labels = jnp.arange(experts, dtype=jnp.int32)
    onehot = (flat[:, None] == labels[None, :]).astype(jnp.int32)
    earlier = jnp.cumsum(onehot, axis=0) - onehot
    position = lax.optimization_barrier(jnp.sum(onehot * (labels[None, :] * capacity + earlier), axis=1))
    slot_ids = jnp.arange(experts * capacity, dtype=jnp.int32)
    table = (position[None, :] == slot_ids[:, None]).astype(jnp.float32).reshape(experts * capacity, count, 2)
    picks = lax.optimization_barrier(jnp.sum(table, axis=2))
    weighted = lax.optimization_barrier(jnp.sum(table * gate_rows[None, :, :], axis=2))
    return (picks, weighted)

def expert_scores(rows_in, rows_back, gate_proj, up_proj, down_proj, input_proj, output_proj, hidden_proj, grad_proj, query_rows):
    gate_pre = jnp.dot(rows_in, gate_proj, preferred_element_type=jnp.float32)
    up_pre = jnp.dot(rows_in, up_proj, preferred_element_type=jnp.float32)
    sigma = jax.nn.sigmoid(gate_pre)
    hidden = (gate_pre * sigma * up_pre).astype(jnp.bfloat16)
    a_input = jnp.dot(rows_in, input_proj, preferred_element_type=jnp.float32)
    a_hidden = jnp.dot(hidden, hidden_proj, preferred_element_type=jnp.float32)
    back = lax.dot_general(rows_back, down_proj, (((1,), (1,)), ((), ())), preferred_element_type=jnp.float32)
    d_up = (back * gate_pre * sigma).astype(jnp.bfloat16)
    d_gate = (back * up_pre * sigma * (1.0 + gate_pre * (1.0 - sigma))).astype(jnp.bfloat16)
    b_output = jnp.dot(rows_back, output_proj, preferred_element_type=jnp.float32)
    b_up = jnp.dot(d_up, grad_proj, preferred_element_type=jnp.float32)
    b_gate = jnp.dot(d_gate, grad_proj, preferred_element_type=jnp.float32)
    height = rows_back.shape[0]
    sketch = jnp.concatenate([(a_hidden[:, :, None] * b_output[:, None, :]).reshape(height, -1), (a_input[:, :, None] * b_up[:, None, :]).reshape(height, -1), (a_input[:, :, None] * b_gate[:, None, :]).reshape(height, -1)], axis=1).astype(jnp.bfloat16)
    return lax.dot_general(sketch, query_rows, (((1,), (1,)), ((), ())), preferred_element_type=jnp.float32)

def reference(inputs, cotangents, routes, gates, w_gate, w_up, w_down, proj_in, proj_out, proj_hid_a, proj_hid_b, queries):
    sources = N_EXPERT
    rows_in = inputs.reshape(sources, TOK_DEV, D)
    rows_back = cotangents.reshape(sources, TOK_DEV, D)
    picks, weighted = jax.vmap(lambda r, g: slot_matrix(r, g, EXPERTS, CAP))(routes.reshape(sources, TOK_DEV, 2), gates.reshape(sources, TOK_DEV, 2))

    def dispatch(index):
        pick = picks[index].astype(jnp.bfloat16)
        first = jnp.dot(pick, rows_in[index], preferred_element_type=jnp.float32).astype(jnp.bfloat16)
        second = jnp.dot(pick, rows_back[index], preferred_element_type=jnp.float32).astype(jnp.bfloat16)
        return (first, second)
    slots_in, slots_back = lax.map(dispatch, jnp.arange(sources, dtype=jnp.int32))
    slots_in = slots_in.reshape(sources, EXPERTS, CAP, D).transpose(1, 0, 2, 3).reshape(EXPERTS, sources * CAP, D)
    slots_back = slots_back.reshape(sources, EXPERTS, CAP, D).transpose(1, 0, 2, 3).reshape(EXPERTS, sources * CAP, D)

    def per_expert(expert):
        return expert_scores(slots_in[expert], slots_back[expert], w_gate[expert], w_up[expert], w_down[expert], proj_in, proj_out, proj_hid_a, proj_hid_b, queries)
    scores = lax.map(per_expert, jnp.arange(EXPERTS, dtype=jnp.int32))
    scores = scores.reshape(EXPERTS, sources, CAP, NQ).transpose(1, 0, 2, 3).reshape(sources, EXPERTS * CAP, NQ)

    def combine(index):
        return lax.dot_general(weighted[index], scores[index], (((0,), (0,)), ((), ())), precision=lax.Precision.HIGHEST, preferred_element_type=jnp.float32)
    token_scores = lax.map(combine, jnp.arange(sources, dtype=jnp.int32)).reshape(TOKENS, NQ)
    query_totals = lax.optimization_barrier(jnp.sum(token_scores, axis=0)) * (1.0 / math.sqrt(TOKENS))
    return (token_scores, query_totals)
```

```python
import functools
import math

import jax
import jax.numpy as jnp
from jax import lax
from jax.experimental import pallas as pl
from jax.experimental.pallas import tpu as pltpu
from jax.sharding import PartitionSpec as P


PLANE = ("dp", "pipe")
F32 = jnp.float32
BF16 = jnp.bfloat16
NT = (((1,), (1,)), ((), ()))


def slot_matrix(route_rows, gate_rows, experts, capacity):
    count = route_rows.shape[0]
    flat = route_rows.reshape(-1)
    labels = jnp.arange(experts, dtype=jnp.int32)
    onehot = (flat[:, None] == labels[None, :]).astype(jnp.int32)
    earlier = jnp.cumsum(onehot, axis=0) - onehot
    position = jnp.sum(onehot * (labels[None, :] * capacity + earlier), axis=1)
    slot_ids = jnp.arange(experts * capacity, dtype=jnp.int32)
    table = (
        (position[None, :] == slot_ids[:, None])
        .astype(jnp.float32)
        .reshape(experts * capacity, count, 2)
    )
    picks = jnp.sum(table, axis=2)
    weighted = jnp.sum(table * gate_rows[None, :, :], axis=2)
    return (picks, weighted)


def slot_body(
    inputs,
    cotangents,
    routes,
    gates,
    w_gate,
    w_up,
    w_down,
    proj_in,
    proj_out,
    proj_hid_a,
    proj_hid_b,
    queries,
):
    experts = lax.axis_size("expert")
    count, width = inputs.shape
    capacity = 4 * count // experts
    query_count = queries.shape[0]
    picks, weighted = slot_matrix(routes, gates, experts, capacity)
    pick_rows = picks.astype(BF16)
    columns = width // lax.axis_size(PLANE)
    start = lax.axis_index(PLANE) * columns

    def dispatch(rows):
        part = lax.dynamic_slice_in_dim(rows, start, columns, 1)
        buffer = jnp.dot(pick_rows, part, preferred_element_type=F32).astype(BF16)
        sent = lax.all_to_all(
            buffer.reshape(experts, capacity, columns),
            "expert",
            split_axis=0,
            concat_axis=0,
            tiled=True,
        )
        return lax.all_gather(sent, PLANE, axis=2, tiled=True).reshape(-1, width)

    slot_in, slot_back = dispatch(inputs), dispatch(cotangents)
    gate_pre = jnp.dot(slot_in, w_gate[0], preferred_element_type=F32)
    up_pre = jnp.dot(slot_in, w_up[0], preferred_element_type=F32)
    sigma = jax.nn.sigmoid(gate_pre)
    hidden = (gate_pre * sigma * up_pre).astype(BF16)
    back = lax.dot_general(slot_back, w_down[0], NT, preferred_element_type=F32)
    d_up = (back * gate_pre * sigma).astype(BF16)
    d_gate = (back * up_pre * sigma * (1.0 + gate_pre * (1.0 - sigma))).astype(BF16)
    a_hidden, b_up, b_gate = lax.psum(
        (
            jnp.dot(hidden, proj_hid_a, preferred_element_type=F32),
            jnp.dot(d_up, proj_hid_b, preferred_element_type=F32),
            jnp.dot(d_gate, proj_hid_b, preferred_element_type=F32),
        ),
        PLANE,
    )
    a_input = jnp.dot(slot_in, proj_in, preferred_element_type=F32)
    b_output = jnp.dot(slot_back, proj_out, preferred_element_type=F32)
    height = slot_in.shape[0]
    sketch = jnp.concatenate(
        [
            (a_hidden[:, :, None] * b_output[:, None, :]).reshape(height, -1),
            (a_input[:, :, None] * b_up[:, None, :]).reshape(height, -1),
            (a_input[:, :, None] * b_gate[:, None, :]).reshape(height, -1),
        ],
        axis=1,
    ).astype(BF16)
    scores = lax.dot_general(sketch, queries, NT, preferred_element_type=F32)
    returned = lax.all_to_all(
        scores.reshape(experts, capacity, query_count),
        "expert",
        split_axis=0,
        concat_axis=0,
        tiled=True,
    )
    token_scores = lax.dot_general(
        weighted,
        returned.reshape(-1, query_count),
        (((0,), (0,)), ((), ())),
        precision=lax.Precision.HIGHEST,
        preferred_element_type=F32,
    )
    scale = 1.0 / math.sqrt(count * experts)
    totals = lax.psum(jnp.sum(token_scores, axis=0), "expert")
    return (token_scores, totals * scale)


def hidden_kernel(blocks, order_ref, *refs):
    n = 1 + max(ref for block in blocks for _, _, *pair in block for ref, _ in pair)
    rows, (wg, wu, wd, pha, phb, out) = refs[:n], refs[n : n + 6]
    xs, gs, wgs, wus, wds, acc_g, acc_u, acc_b, hid, dup, dgate, sems, row_sems = refs[n + 6 :]
    steps, tall, cut = xs.shape
    count = tall // len(blocks)
    core = order_ref[steps]
    ka, kb = pha.shape[0], phb.shape[0]

    moves = [[[], []] for _ in range(steps)]
    for s, block in enumerate(blocks):
        for i, part, *pair in block:
            for kind, (ref, at) in enumerate(pair):
                here = (xs, gs)[kind].at[i, pl.ds(s * count, count)]
                if part is None:
                    there = rows[ref].at[:, pl.ds(pl.multiple_of(order_ref[i] * cut, cut), cut)]
                else:
                    there = rows[ref].at[at]
                    lane = (core if part == 0 else 1 - core) * (cut // 2)
                    here = here.at[:, pl.ds(pl.multiple_of(lane, cut // 2), cut // 2)]
                moves[i][kind].append((there, here))
    copies = []
    for i in range(steps):
        at = pl.ds(pl.multiple_of(order_ref[i] * cut, cut), cut)
        lanes = [
            [(wg.at[0, at], wgs.at[i])],
            moves[i][0],
            [(wu.at[0, at], wus.at[i])],
            moves[i][1],
            [(wd.at[0, :, at], wds.at[i])],
        ]
        made = []
        k = 0
        for lane_no, lane in enumerate(lanes):
            group = []
            for src, dst in lane:
                if lane_no in (1, 3):
                    sem = row_sems.at[i, k]
                    k += 1
                else:
                    sem = sems.at[i, lane_no // 2]
                group.append(pltpu.make_async_copy(src, dst, sem))
            made.append(group)
        copies.append(made)
    for made in copies:
        for group in made:
            for copy in group:
                copy.start()

    def put(acc, i, value):
        if i:
            acc[...] += value
        else:
            acc[...] = value

    for i in range(steps):
        gate_w, x_rows, up_w, g_rows, down_w = copies[i]
        for copy in gate_w + x_rows:
            copy.wait()
        put(acc_g, i, jnp.dot(xs[i], wgs[i], preferred_element_type=F32))
        for copy in up_w:
            copy.wait()
        put(acc_u, i, jnp.dot(xs[i], wus[i], preferred_element_type=F32))
        for copy in g_rows + down_w:
            copy.wait()
        put(acc_b, i, lax.dot_general(gs[i], wds[i], NT, preferred_element_type=F32))

    high = 16

    def nonlinear(i, carry):
        at = pl.ds(pl.multiple_of(i * high, high), high)
        gate, up, back = acc_g[at, :], acc_u[at, :], acc_b[at, :]
        sigma = jax.nn.sigmoid(gate)
        act = gate * sigma
        hid[at, :] = (act * up).astype(BF16)
        dup[at, :] = (back * act).astype(BF16)
        dgate[at, :] = (back * up * sigma * (1.0 + gate * (1.0 - sigma))).astype(BF16)
        return carry

    lax.fori_loop(0, tall // high, nonlinear, 0, unroll=2)
    out[:ka] = lax.dot_general(pha[...], hid[...], NT, preferred_element_type=F32)
    out[ka : ka + kb] = lax.dot_general(phb[...], dup[...], NT, preferred_element_type=F32)
    out[ka + kb :] = lax.dot_general(phb[...], dgate[...], NT, preferred_element_type=F32)


def hidden_call(blocks, rows, order, count, weights):
    w_gate, w_up, w_down, pha, phb = weights
    width, units = w_gate.shape[1:]
    steps = order.shape[0] - 1
    cut = width // steps
    ka, kb = pha.shape[0], phb.shape[0]
    tall = count * len(blocks)
    most = 2 * sum(1 for block in blocks for i, *_ in block if i == 0)
    anywhere = pl.BlockSpec(memory_space=pl.ANY)
    return pl.pallas_call(
        functools.partial(hidden_kernel, blocks),
        in_specs=[pl.BlockSpec(memory_space=pltpu.SMEM)]
        + [anywhere] * (len(rows) + 3)
        + [pl.BlockSpec(memory_space=pltpu.VMEM)] * 2,
        out_specs=pl.BlockSpec(memory_space=pltpu.VMEM),
        out_shape=jax.ShapeDtypeStruct((ka + 2 * kb, tall), F32),
        scratch_shapes=[
            pltpu.VMEM((steps, tall, cut), BF16),
            pltpu.VMEM((steps, tall, cut), BF16),
            pltpu.VMEM((steps, cut, units), BF16),
            pltpu.VMEM((steps, cut, units), BF16),
            pltpu.VMEM((steps, units, cut), BF16),
        ]
        + [pltpu.VMEM((tall, units), F32)] * 3
        + [pltpu.VMEM((tall, units), BF16)] * 3
        + [pltpu.SemaphoreType.DMA((steps, 3)), pltpu.SemaphoreType.DMA((steps, most))],
        cost_estimate=pl.CostEstimate(
            flops=6 * tall * width * units, bytes_accessed=6 * width * units, transcendentals=0
        ),
    )(order, *rows, w_gate, w_up, w_down, pha, phb)


def score_kernel(ka, kb, place_ref, keep_ref, other_ref, q_ref, *refs):
    n = len(refs) // 2
    notes, outs = refs[:n], refs[n:]
    core, z = place_ref[0], place_ref[1]
    keep, other = keep_ref[...], other_ref[...]
    part = jnp.concatenate(
        [jnp.where(core == 0, keep, other), jnp.where(core == 0, other, keep)], axis=1
    )
    full = jnp.concatenate([note[: ka + kb] for note in notes], axis=1)
    scale = jnp.concatenate([note[pl.ds(ka + kb + z, 1), :] for note in notes], axis=1)
    a_hid, b_up, b_gate = part[:ka], part[ka : ka + kb], part[ka + kb :]
    a_in, b_out = full[:ka], full[ka:]
    nq = q_ref.shape[0]
    total = None
    group = 256 // kb
    base = 0
    for a, b in ((a_hid, b_out), (a_in, b_up), (a_in, b_gate)):
        for i in range(0, ka, group):
            block = jnp.concatenate(
                [(a[i + j : i + j + 1] * b).astype(BF16) for j in range(group)], axis=0
            )
            term = jnp.dot(q_ref[:, base : base + group * kb], block, preferred_element_type=F32)
            total = term if total is None else total + term
            base += group * kb
    total = total * scale
    ones = jnp.ones((8, total.shape[1]), F32)
    sums = lax.dot_general(
        ones, total, NT, precision=lax.Precision.HIGHEST, preferred_element_type=F32
    )
    count = outs[0].shape[1]
    sums = jnp.concatenate([sums, jnp.zeros((8, count - nq), F32)], axis=1)
    for s, out in enumerate(outs):
        out[:nq] = total[:, s * count : (s + 1) * count]
        out[nq:] = sums


def last_kernel(scale, place_ref, *refs):
    pieces, (tokens, totals) = refs[:-2], refs[-2:]
    z = place_ref[1]
    n = len(pieces)
    nq = tokens.shape[0]
    tokens[...] = functools.reduce(jnp.add, [p[:nq] for p in pieces])
    sums = [p[nq : nq + 1] for p in pieces]
    total = None
    for e in range(n):
        term = sums[0]
        for s in range(1, n):
            term = jnp.where(lax.rem(z + s, n) == e, sums[s], term)
        total = term if total is None else total + term
    totals[...] = total * scale


def token_body(
    inputs,
    cotangents,
    routes,
    gates,
    w_gate,
    w_up,
    w_down,
    proj_in,
    proj_out,
    proj_hid_a,
    proj_hid_b,
    queries,
):
    experts = lax.axis_size("expert")
    cores = 2
    ys, xs = lax.axis_size("dp") // cores, lax.axis_size("pipe")
    chips = ys * xs
    count, width = inputs.shape
    nq = queries.shape[0]
    ka, kb = proj_hid_a.shape[1], proj_hid_b.shape[1]
    dp, x, z = lax.axis_index("dp"), lax.axis_index("pipe"), lax.axis_index("expert")
    y, core = dp // cores, dp % cores
    cut = width // (chips * cores)

    def over_z(value, shift):
        pairs = [(i, (i + shift) % experts) for i in range(experts)]
        return lax.ppermute(value, "expert", pairs)

    def over_plane(value, dy, dc, dx):
        pairs = []
        for i in range(ys):
            for c in range(cores):
                for k in range(xs):
                    to = (((i + dy) % ys) * cores + (c + dc) % cores) * xs + (k + dx) % xs
                    pairs.append(((i * cores + c) * xs + k, to))
        return lax.ppermute(value, PLANE, pairs)

    def swap(value):
        return over_plane(value, 0, 1, 0)

    offsets = [(dy, dx) for dy in range(ys) for dx in range(xs)]
    chip_at = [((y - dy) % ys) * xs + (x - dx) % xs for dy, dx in offsets]
    order = jnp.stack([*chip_at, core]).astype(jnp.int32)
    place = jnp.stack([core, z]).astype(jnp.int32)
    weights = (w_gate, w_up, w_down, proj_hid_a.T, proj_hid_b.T)

    def piece_of(chip):
        start = (chip * cores + core) * cut
        return jnp.stack(
            [
                lax.dynamic_slice_in_dim(inputs, start, cut, 1),
                lax.dynamic_slice_in_dim(cotangents, start, cut, 1),
            ]
        )

    shifts = list(range(1, experts))
    piece = piece_of(chip_at[0])
    across = len(offsets) - 1 if ys > 1 and xs > 1 else 0
    extra = piece_of(chip_at[across]) if across else None
    came = {}
    for s in shifts:
        came[s] = over_z(piece, s)
    came_extra = over_z(extra, shifts[-1]) if across else None

    labels = jnp.arange(experts, dtype=jnp.int32)
    named = (routes.T[:, None, :] == labels[None, :, None]).astype(F32)
    table = jnp.sum(named * gates.T[:, None, :], axis=0)
    down = (((0,), (1,)), ((), ()))
    note = jnp.concatenate(
        [
            lax.dot_general(proj_in, inputs, down, preferred_element_type=F32),
            lax.dot_general(proj_out, cotangents, down, preferred_element_type=F32),
            table,
        ],
        axis=0,
    )
    notes = [note]
    for s in shifts:
        notes.append(over_z(note, s))

    def spread(s):
        found = []
        for i, (dy, dx) in enumerate(offsets):
            if i == 0:
                near = came[s]
            elif s == shifts[-1] and i == across:
                near = came_extra
            else:
                near = over_plane(came[s], dy, 0, dx)
            found.append((i, near))
        return found

    def block_rows(spreads):
        rows, blocks = [], []
        for near_pieces in spreads:
            block = []
            for i, near in near_pieces:
                for part, array in enumerate((near, swap(near))):
                    block.append((i, part, (len(rows), 0), (len(rows), 1)))
                    rows.append(array)
            blocks.append(block)
        return rows, blocks

    near = {s: spread(s) for s in shifts}
    early = shifts[: experts // 2 - 1]
    late = shifts[experts // 2 - 1 :]
    rows, blocks = block_rows([near[s] for s in early])
    base = len(rows)
    own = [(i, None, (base, 0), (base + 1, 0)) for i in range(chips)]
    first = hidden_call(
        [own] + blocks, [*rows, inputs, cotangents], order, count, weights
    )
    rows, blocks = block_rows([near[s] for s in late])
    second = hidden_call(blocks, rows, order, count, weights)

    keep = jnp.where(core == 0, first, second) + swap(jnp.where(core == 0, second, first))
    sent = keep.astype(BF16)
    for dy, dx in offsets[1:]:
        keep = keep + over_plane(sent, dy, 0, dx).astype(F32)
    other = swap(keep)

    smem = pl.BlockSpec(memory_space=pltpu.SMEM)
    vmem = pl.BlockSpec(memory_space=pltpu.VMEM)
    scored = pl.pallas_call(
        functools.partial(score_kernel, ka, kb),
        in_specs=[smem] + [vmem] * (3 + experts),
        out_specs=[vmem] * experts,
        out_shape=[jax.ShapeDtypeStruct((nq + 8, count), F32)] * experts,
    )(place, keep, other, queries, *notes)
    back = [scored[0]] + [over_z(scored[s], -s) for s in shifts]
    tokens, totals = pl.pallas_call(
        functools.partial(last_kernel, 1.0 / math.sqrt(count * experts)),
        in_specs=[smem] + [vmem] * experts,
        out_specs=[vmem] * 2,
        out_shape=[
            jax.ShapeDtypeStruct((nq, count), F32),
            jax.ShapeDtypeStruct((1, count), F32),
        ],
    )(place, *back)
    return (tokens.T, totals[0, :nq])


def solution(mesh):
    placed = (
        P("expert", None),
        P("expert", None),
        P("expert", None),
        P("expert", None),
        P("expert", None, PLANE),
        P("expert", None, PLANE),
        P("expert", PLANE, None),
        P(),
        P(),
        P(PLANE, None),
        P(PLANE, None),
        P(PLANE, None),
    )

    experts, dp, _ = (mesh.shape[name] for name in ("expert", "dp", "pipe"))
    whole = experts <= 4 and experts % 2 + dp % 2 == 0

    def body(*args):
        if not whole:
            return slot_body(*args)
        return token_body(*args)

    return jax.shard_map(
        body,
        mesh=mesh,
        in_specs=placed,
        out_specs=(P("expert", PLANE), P(PLANE)),
        check_vma=False,
    )
```
